32 devices in a mesh: dp: 8 (over z, y), mp: 4 (over x, core).
Axes of the slice: x: 2, y: 2, z: 4, core: 2. Of those that a mesh axis runs over, the one named last changes fastest.
Arguments:
- logits: bfloat16 [1024, 16384], P('dp', 'mp'), may hold values from -72 to 240
- targets: int32 [1024], P('dp'), may hold values from 0 to 16383
- resp_mask: int32 [1024], P('dp'), may hold values from 0 to 1, as said below
- rewards: int32 [8], P('dp'), may hold values from 0 to 10
- groups: int32 [8], P('dp'), may hold values from 0 to 1, as said below
- unit_grad: bfloat16 [1024, 8192], P(('dp', 'mp')), may hold values from -192 to 192
- mix: bfloat16 [1024, 2048], P('dp', 'mp'), may hold values from -6 to 6
- w_out: bfloat16 [2048, 8192], P('mp', 'dp'), may hold values from -0.125 to 0.125
Outputs:
- token_logprob: float32 [1024], P('dp')
- policy_loss: float32 [], replicated
- grad_mix: bfloat16 [1024, 2048], P('dp', 'mp')
- grad_w_out: bfloat16 [2048, 8192], P('mp', 'dp')
The draws below stay inside these ranges and needn't reach their ends.
Inputs may be any that keep to these rules, and one draw needn't show every extreme that they name: `resp_mask`: in each sample the response mask is a run of ones followed by zeros, with at least 32 ones. `groups`: each prompt id names exactly 4 samples.
All inputs are finite; a program needn't handle non-finite values.
Results may differ from the reference program's by a relative error of at most 0.005.
Values may be sent and summed in bfloat16 or wider, within the bound.
No kernel may reach another device: no remote copies, remote signals or barrier semaphores. Data moves between devices by JAX's collectives and lax.ppermute only.
A program may use at most 64 MiB of HBM per device.

```python
import jax
import jax.numpy as jnp
from jax import lax

D = 8192
K = 4
ROWS = 128
SEQS = 8
PROMPTS = 2
TOKENS = 1024
VOCAB = 16384
QW = 2048


def draw_logits(key, part):
    keys = jax.random.split(key, 1)
    values = 3.0 * jnp.clip(jax.random.normal(keys[0], (TOKENS, VOCAB), jnp.float32), -6.0, 6.0)
    return values.astype(jnp.bfloat16)


def draw_resp_mask(key, part):
    jitter = jax.random.randint(key, (SEQS, 1), 0, ROWS // 8 + 1)
    sample_index = jnp.arange(SEQS, dtype=jnp.int32)[:, None]
    length = jnp.minimum(ROWS // 4 + sample_index * (ROWS * 3 // 4) // SEQS + jitter, ROWS)
    position = jnp.arange(ROWS, dtype=jnp.int32)[None, :]
    return (position < length).astype(jnp.int32).reshape(TOKENS)


def draw_groups(key, part):
    return (jax.random.permutation(key, SEQS) // K).astype(jnp.int32)


def touch_ends(values, key, least, top_value):
    extent = values.shape
    place = [jax.random.randint(jax.random.fold_in(key, axis), (), 0, extent[axis]) for axis in range(len(extent))]
    values = values.at[tuple(place)].set(least)
    longest = extent.index(max(extent))
    place[longest] = (place[longest] + 1) % extent[longest]
    return values.at[tuple(place)].set(top_value)


def block_scale(own_key, shape, pieces, least, high):
    def one(dim, blocks):
        draws = jax.random.uniform(jax.random.fold_in(jax.random.fold_in(own_key, 6), dim), (blocks,), jnp.float32, least / len(pieces), high / len(pieces))
        return jnp.repeat(jnp.exp(draws), shape[dim] // blocks).reshape((-1,) + (1,) * (len(shape) - dim - 1))

    factor_of = one(*pieces[0])
    for cut in pieces[1:]:
        factor_of = factor_of * one(*cut)
    return factor_of


def gaussian(key, dims, width, reach, cuts=(), kind=jnp.bfloat16):
    level = block_scale(key, dims, cuts, -0.22, 0.18) if cuts else 1.0
    array = jax.random.normal(key, dims, jnp.float32) * width * level
    return jnp.minimum(jnp.maximum(array, -reach), reach).astype(kind)


def setup_inputs(seed: int = 0) -> dict:
    key_of = jax.random.split(jax.random.key(seed), 9)
    logits = draw_logits(jax.random.fold_in(key_of[8], 71), 0)
    targets = touch_ends(jax.random.randint(key_of[1], (TOKENS,), 0, VOCAB), jax.random.fold_in(key_of[1], 1), 0, VOCAB - 1).astype(jnp.int32)
    resp_mask = draw_resp_mask(jax.random.fold_in(key_of[8], 71), 0)
    rewards = touch_ends(jax.random.randint(key_of[3], (SEQS,), 0, 11), jax.random.fold_in(key_of[3], 1), 0, 10).astype(jnp.int32)
    groups = draw_groups(jax.random.fold_in(key_of[8], 71), 0)
    unit_grad = gaussian(key_of[5], (TOKENS, D), 32.0, 192.0, ((0, 32),))
    mix = gaussian(key_of[6], (TOKENS, QW), 1.0, 6.0, ((0, 8), (1, 4)))
    w_out = gaussian(key_of[7], (QW, D), QW ** -0.5, 0.125, ((0, 4), (1, 8)))
    return {"logits": logits, "targets": targets, "resp_mask": resp_mask, "rewards": rewards, "groups": groups, "unit_grad": unit_grad, "mix": mix, "w_out": w_out}


def sample_logprob(inputs):
    values, chosen = inputs
    wide = values.astype(jnp.float32)
    highest = jnp.max(wide, axis=1)
    summed = jnp.sum(jnp.exp(wide - highest[:, None]), axis=1)
    picked = jnp.take_along_axis(wide, chosen[:, None].astype(jnp.int32), axis=1)[:, 0]
    return picked - (highest + jnp.log(summed))


def reference(logits, targets, resp_mask, rewards, groups, unit_grad, mix, w_out):
    logprob = lax.map(sample_logprob, (logits.reshape(SEQS, ROWS, VOCAB), targets.reshape(SEQS, ROWS)))
    mask_float = resp_mask.astype(jnp.float32).reshape(SEQS, ROWS)
    token_count = jnp.sum(mask_float)
    reward_float = rewards.astype(jnp.float32)
    member = (groups[:, None] == jnp.arange(PROMPTS, dtype=jnp.int32)[None, :]).astype(jnp.float32)
    group_total = jnp.sum(member * reward_float[:, None], axis=0)
    own_total = jnp.sum(member * group_total[None, :], axis=1)
    advantage = reward_float - (own_total - reward_float) / (K - 1)
    weight = advantage[:, None] * mask_float / token_count
    policy_loss = -jnp.sum(weight * logprob)
    grad_out = (-weight.reshape(TOKENS)[:, None] * unit_grad.astype(jnp.float32)).astype(jnp.bfloat16)
    grad_mix = jnp.dot(grad_out, w_out.T, preferred_element_type=jnp.float32).astype(jnp.bfloat16)
    grad_w_out = jnp.dot(mix.T, grad_out, preferred_element_type=jnp.float32).astype(jnp.bfloat16)
    return logprob.reshape(TOKENS), policy_loss, grad_mix, grad_w_out
```

```python
import jax
import jax.numpy as jnp
from jax import lax
from jax.sharding import PartitionSpec as P

K = 4


def swap(value, axis, mask):
    return lax.ppermute(value, axis, [(k, k ^ mask) for k in range(lax.axis_size(axis))])


def gather_small(value, axis):
    step = 1
    while step < lax.axis_size(axis):
        value = jnp.concatenate([value, swap(value, axis, step)], axis=0)
        step *= 2
    return value


def gather_parts(value, axis):
    parts = {0: value}
    step = lax.axis_size(axis) // 2
    while step:
        parts.update({k ^ step: swap(v, axis, step) for k, v in parts.items()})
        step //= 2
    return [parts[k] for k in range(lax.axis_size(axis))]


def shards(logits, targets, resp_mask, rewards, groups, unit_grad, mix, w_out):
    f32, bf16 = jnp.float32, jnp.bfloat16
    n_dp, n_mp = lax.axis_size("dp"), lax.axis_size("mp")
    half = n_dp // 2
    me, lane = lax.axis_index("dp"), lax.axis_index("mp")
    toks, vocab_dev = logits.shape
    rows, width = unit_grad.shape
    cols = width // n_dp
    heads = mix.shape[1]
    order = lane ^ jnp.arange(n_mp)

    pieces = [
        lax.dynamic_slice(unit_grad, (0, (me ^ r) * cols), (rows, cols)) for r in range(n_dp)
    ]
    got = [pieces[0]] + [swap(pieces[r], "dp", r) for r in range(1, n_dp)]
    near = gather_parts(jnp.stack(got[:half]), "mp")
    far = gather_parts(jnp.stack(got[half:]), "mp")

    mask_float = resp_mask.astype(f32)
    record = jnp.stack(
        [
            mask_float,
            jnp.full((toks,), rewards[0].astype(f32)),
            jnp.full((toks,), groups[0].astype(f32)),
        ]
    )[None]
    records = gather_small(record, "dp")
    count = jnp.sum(records[:, 0])
    reward, group = records[:, 1, 0], records[:, 2, 0]
    own_total = jnp.sum(jnp.where(group == group[0], reward, 0.0))
    advantage = reward[0] - (own_total - reward[0]) / (K - 1)
    weight = advantage * mask_float / count

    local_target = targets - lane * vocab_dev
    wide = logits.astype(f32)
    column = lax.broadcasted_iota(jnp.int32, logits.shape, 1)
    picked = jnp.sum(jnp.where(column == local_target[:, None], wide, 0.0), axis=1)
    top = jnp.max(wide, axis=1)
    total = jnp.sum(jnp.exp(wide - top[:, None]), axis=1)
    stats = gather_small(jnp.stack([top, total, picked])[None], "mp")
    highest = jnp.max(stats[:, 0], axis=0)
    summed = jnp.sum(stats[:, 1] * jnp.exp(stats[:, 0] - highest), axis=0)
    logprob = jnp.sum(stats[:, 2], axis=0) - (highest + jnp.log(summed))
    loss_part = -jnp.sum(weight * logprob)
    policy_loss = jnp.sum(gather_small(jnp.full((1, 128), loss_part), "dp")[:, 0])

    scaled = (mix.astype(f32) * -weight[:, None]).astype(bf16)
    scaled = scaled.reshape(n_mp, rows, heads)[order]
    across = swap(scaled, "dp", half)
    mix_near = [scaled] + [swap(scaled, "dp", r) for r in range(1, half)]
    mix_far = [across] + [swap(across, "dp", r) for r in range(1, half)]

    def partial(parts):
        block = jnp.stack(parts)
        return lax.dot_general(
            block, w_out, (((3,), (1,)), ((), ())), preferred_element_type=f32
        )

    def reduce_near(sums):
        sent = sums.astype(bf16)
        total = sums[:, 0]
        for r in range(1, half):
            total = total + swap(sent[:, r], "dp", r).astype(f32)
        return total

    far_sum = reduce_near(partial(far)).astype(bf16)
    mix_sum = reduce_near(partial(near)) + swap(far_sum, "dp", half).astype(f32)
    grad_mix = (mix_sum[order].reshape(toks, heads) * -weight[:, None]).astype(bf16)

    left = jnp.stack(mix_near + mix_far)
    right = jnp.concatenate([jnp.stack(near), jnp.stack(far)], axis=1)
    grad_w_out = lax.dot_general(
        left.transpose(1, 0, 2, 3).reshape(-1, heads),
        right.reshape(-1, cols),
        (((0,), (0,)), ((), ())),
        preferred_element_type=f32,
    ).astype(bf16)
    return (logprob, policy_loss, grad_mix, grad_w_out)


def solution(mesh):
    return jax.shard_map(
        shards,
        mesh=mesh,
        in_specs=(
            P("dp", "mp"),
            P("dp"),
            P("dp"),
            P("dp"),
            P("dp"),
            P(("dp", "mp"), None),
            P("dp", "mp"),
            P("mp", "dp"),
        ),
        out_specs=(P("dp"), P(), P("dp", "mp"), P("mp", "dp")),
        check_vma=False,
    )
```
